32 devices in a mesh: row: 8 (over z, core), col: 4 (over y, x).
Axes of the slice: x: 2, y: 2, z: 4, core: 2. Of those that a mesh axis runs over, the one named last changes fastest.
Arguments:
- basis: float32 [8192, 1024], P('row', 'col'), may hold values from -6 to 6
- merge_coef: float32 [1024, 4096], P('row', 'col'), may hold values from -0.1875 to 0.1875
- panels: float32 [2, 8192, 256], P(None, ('row', 'col')), may hold values from -0.0625 to 0.0625
- factors: float32 [2, 256, 256], replicated, may hold values from -1 to 1
Outputs:
- vectors: float32 [8192, 4096], P(('row', 'col'))
- wsum: float32 [2, 256], replicated
The draws below stay inside these ranges and needn't reach their ends.
All inputs are finite; a program needn't handle non-finite values.
Results may differ from the reference program's by a relative error of at most 0.0001.
Values sent between devices are 32-bit elements; how exact they have to be, the bound alone decides.
No kernel may reach another device: no remote copies, remote signals or barrier semaphores. Data moves between devices by JAX's collectives and lax.ppermute only.
A program may use at most 128 MiB of HBM per device.

```python
import jax
import jax.numpy as jnp
from jax import lax

K = 1024
NB = 256
ROWS = 8192
NEV = 4096


def levels(own_key, extent, cuts, least, high):
    def one(dim, parts):
        heights = jax.random.uniform(jax.random.fold_in(jax.random.fold_in(own_key, 6), dim), (parts,), jnp.float32, least / len(cuts), high / len(cuts))
        return jnp.repeat(jnp.exp(heights), extent[dim] // parts).reshape((-1,) + (1,) * (len(extent) - dim - 1))

    level = one(*cuts[0])
    for cut in cuts[1:]:
        level = level * one(*cut)
    return level


def normal_values(rng, dims, spread, reach, pieces=(), held_as=jnp.bfloat16):
    entries = spread * jax.random.normal(rng, dims, jnp.float32)
    if pieces:
        entries = entries * levels(rng, dims, pieces, -0.22, 0.18)
    return jnp.clip(entries, -reach, reach).astype(held_as)


def setup_inputs(seed: int = 0) -> dict:
    arg_keys = jax.random.split(jax.random.key(seed), 5)
    basis = normal_values(arg_keys[0], (ROWS, K), 1.0, 6.0, ((0, 8), (1, 4)), jnp.float32)
    merge_coef = normal_values(arg_keys[1], (K, NEV), K ** -0.5, 0.1875, ((0, 8), (1, 4)), jnp.float32)
    panels = normal_values(arg_keys[2], (2, ROWS, NB), ROWS ** -0.5, 0.0625, ((1, 32),), jnp.float32)
    factors = normal_values(arg_keys[3], (2, NB, NB), (max(1, 4 * NB * NB // ROWS)) ** -0.5, 1.0, (), jnp.float32)
    return {"basis": basis, "merge_coef": merge_coef, "panels": panels, "factors": factors}


HI = lax.Precision.HIGHEST

def reference(basis, merge_coef, panels, factors):
    x = jnp.dot(basis, merge_coef, precision=HI, preferred_element_type=jnp.float32)
    totals = []
    for index in range(2):
        vecs = panels[index]
        upper = jnp.triu(factors[index])
        proj = jnp.dot(vecs.T, x, precision=HI, preferred_element_type=jnp.float32)
        totals.append(lax.optimization_barrier(jnp.sum(proj, axis=1)) / jnp.sqrt(jnp.float32(NEV)))
        scaled = jnp.dot(upper, proj, precision=HI, preferred_element_type=jnp.float32)
        x = x - jnp.dot(vecs, scaled, precision=HI, preferred_element_type=jnp.float32)
    return (x, jnp.stack(totals))
```

```python
import jax
import jax.numpy as jnp
from jax import lax
from jax.experimental import pallas as pl
from jax.experimental.pallas import tpu as pltpu
from jax.sharding import PartitionSpec as P


HI = lax.Precision.HIGHEST
BOTH = ("row", "col")


def dot(left, right):
    return jnp.dot(left, right, precision=HI, preferred_element_type=jnp.float32)


def dot_t(left, right):
    return lax.dot_general(left, right, (((0,), (0,)), ((), ())), precision=HI, preferred_element_type=jnp.float32)


def masks(bits, core):
    order = list(range(bits)) if core == 0 else list(range(bits))[::-1]
    out = [0]
    for b in order:
        out = out + [m ^ (1 << b) for m in out]
    return out


def split3(x):
    hi = x.astype(jnp.bfloat16)
    return hi, (x - hi.astype(jnp.float32)).astype(jnp.bfloat16)


def product_kernel(n_col, n_z, groups, rows, kb, width, blk, *refs):
    n_pieces = len(groups) * n_col * 2
    idx = refs[0]
    b2 = refs[1 : 1 + n_col]
    pieces = refs[1 + n_col : 1 + n_col + n_pieces]
    out = refs[1 + n_col + n_pieces]
    cbuf, obuf, bhi, blo, in_sem, out_sem = refs[2 + n_col + n_pieces :]
    half = len(groups) * n_col

    def fetch(s, slot):
        copies = []
        for g, zslots in enumerate(groups):
            for side in range(2):
                ref = pieces[side * half + g * n_col + s]
                for i, z in enumerate(zslots):
                    at = pl.multiple_of(idx[side, 64 + z] * blk, blk)
                    n = len(copies)
                    copies.append(
                        pltpu.make_async_copy(
                            ref.at[pl.ds(i * blk, blk), :],
                            cbuf.at[slot, pl.ds(at, blk), :],
                            in_sem.at[slot, n],
                        )
                    )
        return copies

    def store(s, slot):
        at = pl.multiple_of(idx[0, s] * width, width)
        return pltpu.make_async_copy(obuf.at[slot], out.at[:, pl.ds(at, width)], out_sem.at[slot])

    for cp in fetch(0, 0):
        cp.start()
    for s in range(n_col):
        hi, lo = split3(b2[s][...])
        at = pl.multiple_of(idx[0, s] * kb, kb)
        bhi[:, pl.ds(at, kb)] = hi
        blo[:, pl.ds(at, kb)] = lo
    tile = 256
    for s in range(n_col):
        slot = s % 2
        if s + 1 < n_col:
            for cp in fetch(s + 1, 1 - slot):
                cp.start()
        for cp in fetch(s, slot):
            cp.wait()
        if s >= 2:
            store(s - 2, slot).wait()

        @pl.loop(0, width // tile)
        def _(t, slot=slot):
            cols = pl.ds(pl.multiple_of(t * tile, tile), tile)
            hi, lo = split3(cbuf[slot, :, cols])
            acc = jnp.dot(bhi[...], hi, preferred_element_type=jnp.float32)
            acc += jnp.dot(bhi[...], lo, preferred_element_type=jnp.float32)
            acc += jnp.dot(blo[...], hi, preferred_element_type=jnp.float32)
            obuf[slot, :, cols] = acc

        store(s, slot).start()
    for s in range(max(0, n_col - 2), n_col):
        store(s, s % 2).wait()


def product(table, b2, pieces, groups, n_col, n_z):
    rows, kb = b2[0].shape
    blk, width = pieces[0].shape
    depth = kb * n_col
    anywhere = pl.BlockSpec(memory_space=pl.ANY)
    n_in = sum(len(g) for g in groups) * 2

    def body(*refs):
        product_kernel(n_col, n_z, groups, rows, kb, width, blk, *refs)

    return pl.pallas_call(
        body,
        out_shape=jax.ShapeDtypeStruct((rows, width * n_col), jnp.float32),
        in_specs=[pl.BlockSpec(memory_space=pltpu.SMEM)]
        + [pl.BlockSpec(memory_space=pltpu.VMEM)] * n_col
        + [anywhere] * len(pieces),
        out_specs=anywhere,
        scratch_shapes=[
            pltpu.VMEM((2, depth, width), jnp.float32),
            pltpu.VMEM((2, rows, width), jnp.float32),
            pltpu.VMEM((rows, depth), jnp.bfloat16),
            pltpu.VMEM((rows, depth), jnp.bfloat16),
            pltpu.SemaphoreType.DMA((2, n_in)),
            pltpu.SemaphoreType.DMA((2,)),
        ],
        compiler_params=pltpu.CompilerParams(vmem_limit_bytes=24 * 2**20),
        cost_estimate=pl.CostEstimate(flops=6 * rows * depth * width * n_col, bytes_accessed=4 * (depth + rows) * width * n_col, transcendentals=0),
        name="product",
    )(table, *b2, *pieces)


def solution(mesh):
    n_row, n_col = mesh.shape["row"], mesh.shape["col"]
    n_z = n_row // 2
    col_bits, z_bits = n_col.bit_length() - 1, n_z.bit_length() - 1
    col_masks = [masks(col_bits, core) for core in range(2)]
    z_masks = [masks(z_bits, core) for core in range(2)]
    col_twin = [col_masks[1].index(m) for m in col_masks[0]]

    def everyone(to):
        return [(r * n_col + c, to(r, c)) for r in range(n_row) for c in range(n_col)]

    def over_col(x, slot):
        return lax.ppermute(x, BOTH, everyone(lambda r, c: r * n_col + (c ^ col_masks[r % 2][slot])))

    def over_z(x, slot):
        return lax.ppermute(x, BOTH, everyone(lambda r, c: (r ^ (2 * z_masks[r % 2][slot])) * n_col + c))

    def over_core(x):
        return lax.ppermute(x, BOTH, everyone(lambda r, c: (r ^ 1) * n_col + c))

    def per_device(basis, coef, panels, factors):
        row, col = lax.axis_index("row"), lax.axis_index("col")
        core = row % 2
        nb = panels.shape[2]
        part = panels.shape[1]
        kb = basis.shape[1]
        blk = coef.shape[0]

        def by_core(values):
            return jnp.where(core == 0, jnp.array(values[0], jnp.int32), jnp.array(values[1], jnp.int32))

        cols_of = col ^ by_core(col_masks)
        rows_of = ((row // 2) ^ by_core(z_masks)) * 2 + core

        sums = jnp.sum(coef, axis=1)
        lanes = 2 * nb
        extra = jnp.zeros((8, lanes), jnp.float32).at[0, :blk].set(sums)
        held = jnp.concatenate([panels[0], panels[1]], axis=1)
        held = jnp.concatenate([held, extra], axis=0)
        chunks = [held]
        for step in range(col_bits):
            chunks = chunks + [over_col(x, 2**step) for x in chunks]

        zparts, groups, z_held = [coef], [[0]], coef
        for step in range(z_bits):
            got = over_z(z_held, 2**step)
            groups.append(list(range(2**step, 2 ** (step + 1))))
            zparts.append(got)
            if step + 1 < z_bits:
                z_held = jnp.concatenate([z_held, got], axis=0)
        pieces, others = [], []
        for part_z in zparts:
            found = [part_z]
            for step in range(col_bits):
                found = found + [over_col(x, 2**step) for x in found]
            pieces.append(found)
            others.append([over_core(x) for x in found])

        blocks = [lax.dynamic_slice_in_dim(basis, cols_of[s] * part, part, 0) for s in range(n_col)]
        field = jnp.concatenate(blocks, axis=0)
        vecs = jnp.concatenate([x[:part] for x in chunks], axis=0)
        proj = dot_t(vecs, field)
        cross = dot_t(vecs[:, nb:], vecs[:, :nb])
        row_sum = sum(x[part, :blk] for x in chunks)
        spread = jnp.where(lax.broadcasted_iota(jnp.int32, (n_row, blk), 0) == row, row_sum[None, :], 0.0).reshape(-1)
        spread = jnp.zeros((8 * kb,), jnp.float32).at[: n_row * blk].set(spread).reshape(8, kb)
        cross = jnp.concatenate([cross[:, i : i + kb] for i in range(0, nb, kb)], axis=0)
        total = jnp.concatenate([proj, cross, spread], axis=0)
        half = kb // 2
        mine = lax.dynamic_slice_in_dim(total, core * half, half, 1)
        mine = mine + over_core(lax.dynamic_slice_in_dim(total, (1 - core) * half, half, 1))
        for step in range(z_bits):
            mine = mine + over_z(mine, 2**step)
        theirs = over_core(mine)
        total = jnp.where(core == 0, jnp.concatenate([mine, theirs], 1), jnp.concatenate([theirs, mine], 1))
        proj_one, proj_two = total[:nb], total[nb : 2 * nb]
        cross = jnp.concatenate([total[i : i + nb] for i in range(2 * nb, total.shape[0] - 8, nb)], axis=1)
        weight = total[-8:].reshape(-1)
        upper = jnp.triu(factors)
        scaled = dot(upper[0], proj_one)
        proj_two = proj_two - dot(cross, scaled)
        both = jnp.concatenate([scaled, dot(upper[1], proj_two)], axis=0)
        field = field - dot(vecs, both)
        weight = lax.dynamic_slice_in_dim(weight, col * kb, kb, 0)
        share = jnp.sum(jnp.concatenate([proj_one, proj_two], axis=0) * weight[None, :], axis=1).reshape(2, nb)

        tail = jnp.zeros((8, kb), jnp.float32).at[: 2 * nb // kb].set(share.reshape(-1, kb))
        sends = [jnp.concatenate([field[s * part : (s + 1) * part], tail], axis=0) for s in range(n_col)]
        tall = [sends[0]] + [over_col(sends[s], s) for s in range(1, n_col)]
        shares = [x[part : part + 2 * nb // kb].reshape(2, nb) for x in tall]
        by_mask = [
            jnp.where(core == 0, shares[col_masks[0].index(m)], shares[col_masks[1].index(m)]) for m in range(n_col)
        ]
        while len(by_mask) > 1:
            by_mask = [by_mask[i] + by_mask[i + 1] for i in range(0, len(by_mask), 2)]
        width = coef.shape[1]
        wsum = by_mask[0] / jnp.sqrt(jnp.float32(width * n_col))

        twin_rows = ((row // 2) ^ by_core(z_masks[::-1])) * 2 + (1 - core)
        table = jnp.zeros((2, 128), jnp.int32)
        table = table.at[0, :n_col].set(cols_of).at[0, 64 : 64 + n_z].set(rows_of).at[1, 64 : 64 + n_z].set(twin_rows)
        flat = [x for g in pieces for x in g] + [others[g][col_twin[s]] for g in range(len(groups)) for s in range(n_col)]
        vectors = product(table, [x[:part] for x in tall], flat, groups, n_col, n_z)
        return vectors, wsum

    placed = (P("row", "col"), P("row", "col"), P(None, ("row", "col"), None), P())
    return jax.shard_map(
        per_device,
        mesh=mesh,
        in_specs=placed,
        out_specs=(P(("row", "col"), None), P()),
        check_vma=False,
    )
```

```python
import jax
import jax.numpy as jnp
from jax import lax
from jax.experimental import pallas as pl
from jax.experimental.pallas import tpu as pltpu
from jax.sharding import PartitionSpec as P


BOTH = ("row", "col")


F32 = jnp.float32
ROWS_ROWS = (((0,), (0,)), ((), ()))
COLS_COLS = (((1,), (1,)), ((), ()))
PLAIN = (((1,), (0,)), ((), ()))


def masks(bits, core):
    order = list(range(bits)) if core == 0 else list(range(bits))[::-1]
    out = [0]
    for b in order:
        out = out + [m ^ (1 << b) for m in out]
    return out


def split3(x):
    hi = x.astype(jnp.bfloat16)
    return hi, (x - hi.astype(F32)).astype(jnp.bfloat16)


def mul(left, right, dims=PLAIN):
    def one(a, b):
        return lax.dot_general(a, b, dims, preferred_element_type=F32)

    return one(left[0], right[0]) + (one(left[0], right[1]) + one(left[1], right[0]))


def pick(core, pair):
    return jnp.where(core == 0, pair[0], pair[1])


class Plan:
    def __init__(self, mesh):
        self.n_row, self.n_col = mesh.shape["row"], mesh.shape["col"]
        self.n_z = self.n_row // 2
        self.col_bits, self.z_bits = self.n_col.bit_length() - 1, self.n_z.bit_length() - 1
        self.col_masks = [masks(self.col_bits, core) for core in range(2)]
        self.z_masks = [masks(self.z_bits, core) for core in range(2)]
        self.col_twin = [self.col_masks[1].index(m) for m in self.col_masks[0]]
        self.groups = [[0]] + [list(range(2**b, 2 ** (b + 1))) for b in range(self.z_bits)]

    def place(self):
        row, col = lax.axis_index("row"), lax.axis_index("col")
        return row // 2, lax.rem(row, 2), col

    def col_of(self, col, core, slot):
        return col ^ pick(core, [m[slot] for m in self.col_masks])

    def z_of(self, z, core, slot):
        return z ^ pick(core, [m[slot] for m in self.z_masks])

    def permute(self, x, to):
        pairs = [(r * self.n_col + c, to(r, c)) for r in range(self.n_row) for c in range(self.n_col)]
        return lax.ppermute(x, BOTH, pairs)

    def over_col(self, x, slot):
        return self.permute(x, lambda r, c: r * self.n_col + (c ^ self.col_masks[r % 2][slot]))

    def over_z(self, x, slot):
        return self.permute(x, lambda r, c: (r ^ (2 * self.z_masks[r % 2][slot])) * self.n_col + c)

    def over_core(self, x):
        return self.permute(x, lambda r, c: (r ^ 1) * self.n_col + c)


def project(plan, basis, vecs, sums):
    n_col, kb = plan.n_col, basis.shape[1]
    part, nb = vecs[0].shape[1:]
    half = kb // 2
    blk = sums.shape[1]
    cuts = nb // kb
    height = (2 + cuts) * nb + 8

    def body(basis_ref, sums_ref, *refs):
        v, (keep, send, total) = refs[:n_col], refs[n_col:]
        z, core, col = plan.place()
        proj, cross = [0.0, 0.0], 0.0
        for s in range(n_col):
            at = pl.multiple_of(plan.col_of(col, core, s) * part, part)
            b = split3(basis_ref[pl.ds(at, part), :])
            v0, v1 = split3(v[s][0]), split3(v[s][1])
            proj[0] += mul(v0, b, ROWS_ROWS)
            proj[1] += mul(v1, b, ROWS_ROWS)
            cross += mul(v1, v0, ROWS_ROWS)
        total[:nb, :] = proj[0]
        total[nb : 2 * nb, :] = proj[1]
        for i in range(cuts):
            total[(2 + i) * nb : (3 + i) * nb, :] = cross[:, i * kb : (i + 1) * kb]
        per = kb // blk if kb >= blk else 1
        line = lax.broadcasted_iota(jnp.int32, (8, kb), 0) * per + lax.broadcasted_iota(jnp.int32, (8, kb), 1) // blk
        wide = jnp.concatenate([sums_ref[:1, :]] * per, axis=1)
        total[height - 8 :, :] = jnp.where(line == z * 2 + core, jnp.broadcast_to(wide, (8, kb)), 0.0)
        left, right = total[:, :half], total[:, half:]
        keep[...] = jnp.where(core == 0, left, right)
        send[...] = jnp.where(core == 0, right, left)

    out = jax.ShapeDtypeStruct((height, half), F32)
    return pl.pallas_call(
        body,
        out_shape=(out, out),
        scratch_shapes=[pltpu.VMEM((height, kb), F32)],
        compiler_params=pltpu.CompilerParams(vmem_limit_bytes=16 * 2**20),
        cost_estimate=pl.CostEstimate(flops=36 * part * n_col * nb * kb, bytes_accessed=4 * (3 * part * n_col * kb + height * kb), transcendentals=0),
        name="project",
    )(basis, sums, *vecs)


def update(plan, basis, vecs, factors, mine, theirs):
    n_col, kb = plan.n_col, basis.shape[1]
    part, nb = vecs[0].shape[1:]
    height, _ = mine.shape
    cuts = nb // kb
    tail = 8

    def body(basis_ref, factors_ref, mine_ref, theirs_ref, *refs):
        v, outs = refs[:n_col], refs[n_col:]
        _, core, col = plan.place()
        left = jnp.where(core == 0, mine_ref[...], theirs_ref[...])
        right = jnp.where(core == 0, theirs_ref[...], mine_ref[...])
        total = jnp.concatenate([left, right], axis=1)
        keep = lax.broadcasted_iota(jnp.int32, (nb, nb), 0) <= lax.broadcasted_iota(jnp.int32, (nb, nb), 1)
        upper = [split3(jnp.where(keep, factors_ref[i], 0.0)) for i in range(2)]
        one, two = total[:nb], total[nb : 2 * nb]
        cross = jnp.concatenate([total[(2 + i) * nb : (3 + i) * nb] for i in range(cuts)], axis=1)
        first = mul(upper[0], split3(one))
        split_first = split3(first)
        two = two - mul(split3(cross), split_first)
        split_second = split3(mul(upper[1], split3(two)))
        line = lax.broadcasted_iota(jnp.int32, (8, kb), 0)
        weight = jnp.sum(jnp.where(line == col, total[height - 8 :], 0.0), axis=0, keepdims=True)
        weight = split3(jnp.broadcast_to(weight, (8, kb)))
        shares = [mul(weight, split3(g), COLS_COLS)[:1] for g in (one, two)]
        shares = [x[:, i * kb : (i + 1) * kb] for x in shares for i in range(cuts)]
        shares = jnp.concatenate(shares + [jnp.zeros((tail - 2 * cuts, kb), F32)], axis=0)
        for s in range(n_col):
            at = pl.multiple_of(plan.col_of(col, core, s) * part, part)
            b = basis_ref[pl.ds(at, part), :]
            b = b - mul(split3(v[s][0]), split_first) - mul(split3(v[s][1]), split_second)
            outs[s][:part, :] = b
            outs[s][part:, :] = shares

    out = jax.ShapeDtypeStruct((part + tail, kb), F32)
    return pl.pallas_call(
        body,
        out_shape=(out,) * n_col,
        compiler_params=pltpu.CompilerParams(vmem_limit_bytes=16 * 2**20),
        cost_estimate=pl.CostEstimate(flops=12 * part * n_col * nb * kb, bytes_accessed=4 * (4 * part * n_col * kb + height * kb), transcendentals=0),
        name="update",
    )(basis, factors, mine, theirs, *vecs)


def product(plan, b2, pieces, others):
    n_col, groups = plan.n_col, plan.groups
    kb = b2[0].shape[1]
    rows = b2[0].shape[0] - 8
    blk, width = pieces[0][0].shape
    depth = kb * n_col
    tile = 256
    flat = [x for g in pieces for x in g] + [x for g in others for x in g]
    half = len(groups) * n_col

    def body(*refs):
        b, c = refs[:n_col], refs[n_col : n_col + 2 * half]
        out, cbuf, obuf, bhi, blo, in_sem, out_sem = refs[n_col + 2 * half :]
        z, core, col = plan.place()

        def fetch(s, slot):
            copies = []
            for side in range(2):
                who = core if side == 0 else 1 - core
                t = s if side == 0 else plan.col_twin[s]
                for g, zslots in enumerate(groups):
                    for i, zslot in enumerate(zslots):
                        at = pl.multiple_of((plan.z_of(z, who, zslot) * 2 + who) * blk, blk)
                        copies.append(
                            pltpu.make_async_copy(
                                c[side * half + g * n_col + t].at[pl.ds(i * blk, blk), :],
                                cbuf.at[slot, pl.ds(at, blk), :],
                                in_sem.at[slot, len(copies)],
                            )
                        )
            return copies

        def store(s, slot):
            at = pl.multiple_of(plan.col_of(col, core, s) * width, width)
            return pltpu.make_async_copy(obuf.at[slot], out.at[:, pl.ds(at, width)], out_sem.at[slot])

        for cp in fetch(0, 0):
            cp.start()
        for s in range(n_col):
            hi, lo = split3(b[s][:rows, :])
            at = pl.multiple_of(plan.col_of(col, core, s) * kb, kb)
            bhi[:, pl.ds(at, kb)] = hi
            blo[:, pl.ds(at, kb)] = lo
        for s in range(n_col):
            slot = s % 2
            if s + 1 < n_col:
                for cp in fetch(s + 1, 1 - slot):
                    cp.start()
            for cp in fetch(s, slot):
                cp.wait()
            if s >= 2:
                store(s - 2, slot).wait()

            @pl.loop(0, width // tile)
            def _(t, slot=slot):
                cols = pl.ds(pl.multiple_of(t * tile, tile), tile)
                obuf[slot, :, cols] = mul((bhi[...], blo[...]), split3(cbuf[slot, :, cols]))

            store(s, slot).start()
        for s in range(max(0, n_col - 2), n_col):
            store(s, s % 2).wait()

    anywhere = pl.BlockSpec(memory_space=pl.ANY)
    return pl.pallas_call(
        body,
        out_shape=jax.ShapeDtypeStruct((rows, width * n_col), F32),
        in_specs=[pl.BlockSpec(memory_space=pltpu.VMEM)] * n_col + [anywhere] * len(flat),
        out_specs=anywhere,
        scratch_shapes=[
            pltpu.VMEM((2, depth, width), F32),
            pltpu.VMEM((2, rows, width), F32),
            pltpu.VMEM((rows, depth), jnp.bfloat16),
            pltpu.VMEM((rows, depth), jnp.bfloat16),
            pltpu.SemaphoreType.DMA((2, 2 * plan.n_z)),
            pltpu.SemaphoreType.DMA((2,)),
        ],
        compiler_params=pltpu.CompilerParams(vmem_limit_bytes=24 * 2**20),
        cost_estimate=pl.CostEstimate(flops=6 * rows * depth * width * n_col, bytes_accessed=4 * (depth + rows) * width * n_col, transcendentals=0),
        name="product",
    )(*b2, *flat)


def spread(plan, x):
    found = [x]
    for step in range(plan.col_bits):
        found = found + [plan.over_col(y, 2**step) for y in found]
    return found


def solution(mesh):
    plan = Plan(mesh)

    def per_device(basis, coef, panels, factors):
        nb, kb = panels.shape[2], basis.shape[1]
        part = panels.shape[1]
        n_col, z_bits = plan.n_col, plan.z_bits
        _, core, _ = plan.place()

        vecs = spread(plan, panels)
        sums = jnp.broadcast_to(jnp.sum(coef, axis=1)[None, :], (8, coef.shape[0]))
        for step in range(plan.col_bits):
            sums = sums + plan.over_col(sums, 2**step)

        parts, held = [coef], coef
        for step in range(z_bits):
            got = plan.over_z(held, 2**step)
            parts.append(got)
            if step + 1 < z_bits:
                held = jnp.concatenate([held, got], axis=0)
        pieces = [spread(plan, x) for x in parts]
        others = [[plan.over_core(x) for x in found] for found in pieces]

        keep, send = project(plan, basis, vecs, sums)
        mine = keep + plan.over_core(send)
        for step in range(z_bits):
            mine = mine + plan.over_z(mine, 2**step)
        theirs = plan.over_core(mine)
        sends = update(plan, basis, vecs, factors, mine, theirs)

        tall = [sends[0]] + [plan.over_col(sends[s], s) for s in range(1, n_col)]
        shares = [x[part : part + 2 * nb // kb].reshape(2, nb) for x in tall]
        by_mask = [pick(core, [shares[m.index(i)] for m in plan.col_masks]) for i in range(n_col)]
        while len(by_mask) > 1:
            by_mask = [by_mask[i] + by_mask[i + 1] for i in range(0, len(by_mask), 2)]
        wsum = by_mask[0] / jnp.sqrt(F32(coef.shape[1] * n_col))
        return product(plan, tall, pieces, others), wsum

    placed = (P("row", "col"), P("row", "col"), P(None, ("row", "col"), None), P())
    return jax.shard_map(
        per_device,
        mesh=mesh,
        in_specs=placed,
        out_specs=(P(("row", "col"), None), P()),
        check_vma=False,
    )
```

```python
import jax
import jax.numpy as jnp
from jax import lax
from jax.experimental import pallas as pl
from jax.experimental.pallas import tpu as pltpu
from jax.sharding import PartitionSpec as P


BOTH = ("row", "col")


F32 = jnp.float32
ROWS_ROWS = (((0,), (0,)), ((), ()))
COLS_COLS = (((1,), (1,)), ((), ()))
PLAIN = (((1,), (0,)), ((), ()))


def masks(bits, core):
    order = list(range(bits)) if core == 0 else list(range(bits))[::-1]
    out = [0]
    for b in order:
        out = out + [m ^ (1 << b) for m in out]
    return out


def split3(x):
    hi = x.astype(jnp.bfloat16)
    return hi, (x - hi.astype(F32)).astype(jnp.bfloat16)


def mul(left, right, dims=PLAIN):
    def one(a, b):
        return lax.dot_general(a, b, dims, preferred_element_type=F32)

    return one(left[0], right[0]) + (one(left[0], right[1]) + one(left[1], right[0]))


def pick(core, pair):
    return jnp.where(core == 0, pair[0], pair[1])


class Plan:
    def __init__(self, mesh):
        self.n_row, self.n_col = mesh.shape["row"], mesh.shape["col"]
        self.n_z = self.n_row // 2
        self.col_bits, self.z_bits = self.n_col.bit_length() - 1, self.n_z.bit_length() - 1
        self.col_masks = [masks(self.col_bits, core) for core in range(2)]
        self.z_masks = [masks(self.z_bits, core) for core in range(2)]
        self.col_twin = [self.col_masks[1].index(m) for m in self.col_masks[0]]

    def relayed(self, slot):
        return self.n_z > 2 and self.n_col > 2 and slot == self.n_z // 2

    def place(self):
        row, col = lax.axis_index("row"), lax.axis_index("col")
        return row // 2, lax.rem(row, 2), col

    def col_of(self, col, core, slot):
        return col ^ pick(core, [m[slot] for m in self.col_masks])

    def z_of(self, z, core, slot):
        return z ^ pick(core, [m[slot] for m in self.z_masks])

    def permute(self, x, to):
        pairs = [(r * self.n_col + c, to(r, c)) for r in range(self.n_row) for c in range(self.n_col)]
        return lax.ppermute(x, BOTH, pairs)

    def over_col(self, x, slot):
        return self.permute(x, lambda r, c: r * self.n_col + (c ^ self.col_masks[r % 2][slot]))

    def over_z(self, x, slot):
        return self.permute(x, lambda r, c: (r ^ (2 * self.z_masks[r % 2][slot])) * self.n_col + c)

    def over_core(self, x):
        return self.permute(x, lambda r, c: (r ^ 1) * self.n_col + c)


def project(plan, basis, vecs, sums):
    n_col, kb = plan.n_col, basis.shape[1]
    part, nb = vecs[0].shape[1:]
    half = kb // 2
    blk = sums.shape[1]
    cuts = nb // kb
    height = (2 + cuts) * nb + 8

    def body(basis_ref, sums_ref, *refs):
        v, (keep, send, total) = refs[:n_col], refs[n_col:]
        z, core, col = plan.place()
        proj, cross = [0.0, 0.0], 0.0
        for s in range(n_col):
            at = pl.multiple_of(plan.col_of(col, core, s) * part, part)
            b = split3(basis_ref[pl.ds(at, part), :])
            v0, v1 = split3(v[s][0]), split3(v[s][1])
            proj[0] += mul(v0, b, ROWS_ROWS)
            proj[1] += mul(v1, b, ROWS_ROWS)
            cross += mul(v1, v0, ROWS_ROWS)
        total[:nb, :] = proj[0]
        total[nb : 2 * nb, :] = proj[1]
        for i in range(cuts):
            total[(2 + i) * nb : (3 + i) * nb, :] = cross[:, i * kb : (i + 1) * kb]
        per = kb // blk if kb >= blk else 1
        line = lax.broadcasted_iota(jnp.int32, (8, kb), 0) * per + lax.broadcasted_iota(jnp.int32, (8, kb), 1) // blk
        wide = jnp.concatenate([sums_ref[:1, :]] * per, axis=1)
        total[height - 8 :, :] = jnp.where(line == z * 2 + core, jnp.broadcast_to(wide, (8, kb)), 0.0)
        left, right = total[:, :half], total[:, half:]
        keep[...] = jnp.where(core == 0, left, right)
        send[...] = jnp.where(core == 0, right, left)

    out = jax.ShapeDtypeStruct((height, half), F32)
    return pl.pallas_call(
        body,
        out_shape=(out, out),
        scratch_shapes=[pltpu.VMEM((height, kb), F32)],
        compiler_params=pltpu.CompilerParams(vmem_limit_bytes=16 * 2**20),
        cost_estimate=pl.CostEstimate(flops=36 * part * n_col * nb * kb, bytes_accessed=4 * (3 * part * n_col * kb + height * kb), transcendentals=0),
        name="project",
    )(basis, sums, *vecs)


def update(plan, basis, vecs, factors, mine, theirs):
    n_col, kb = plan.n_col, basis.shape[1]
    part, nb = vecs[0].shape[1:]
    height, _ = mine.shape
    cuts = nb // kb
    tail = 8

    def body(basis_ref, factors_ref, mine_ref, theirs_ref, *refs):
        v, outs = refs[:n_col], refs[n_col:]
        _, core, col = plan.place()
        left = jnp.where(core == 0, mine_ref[...], theirs_ref[...])
        right = jnp.where(core == 0, theirs_ref[...], mine_ref[...])
        total = jnp.concatenate([left, right], axis=1)
        keep = lax.broadcasted_iota(jnp.int32, (nb, nb), 0) <= lax.broadcasted_iota(jnp.int32, (nb, nb), 1)
        upper = [split3(jnp.where(keep, factors_ref[i], 0.0)) for i in range(2)]
        one, two = total[:nb], total[nb : 2 * nb]
        cross = jnp.concatenate([total[(2 + i) * nb : (3 + i) * nb] for i in range(cuts)], axis=1)
        first = mul(upper[0], split3(one))
        split_first = split3(first)
        two = two - mul(split3(cross), split_first)
        split_second = split3(mul(upper[1], split3(two)))
        line = lax.broadcasted_iota(jnp.int32, (8, kb), 0)
        weight = jnp.sum(jnp.where(line == col, total[height - 8 :], 0.0), axis=0, keepdims=True)
        weight = split3(jnp.broadcast_to(weight, (8, kb)))
        shares = [mul(weight, split3(g), COLS_COLS)[:1] for g in (one, two)]
        shares = [x[:, i * kb : (i + 1) * kb] for x in shares for i in range(cuts)]
        shares = jnp.concatenate(shares + [jnp.zeros((tail - 2 * cuts, kb), F32)], axis=0)
        for s in range(n_col):
            at = pl.multiple_of(plan.col_of(col, core, s) * part, part)
            b = basis_ref[pl.ds(at, part), :]
            b = b - mul(split3(v[s][0]), split_first) - mul(split3(v[s][1]), split_second)
            outs[s][:part, :] = b
            outs[s][part:, :] = shares

    out = jax.ShapeDtypeStruct((part + tail, kb), F32)
    return pl.pallas_call(
        body,
        out_shape=(out,) * n_col,
        compiler_params=pltpu.CompilerParams(vmem_limit_bytes=16 * 2**20),
        cost_estimate=pl.CostEstimate(flops=12 * part * n_col * nb * kb, bytes_accessed=4 * (4 * part * n_col * kb + height * kb), transcendentals=0),
        name="update",
    )(basis, factors, mine, theirs, *vecs)


def product(plan, b2, pieces, others, slots, base=None):
    n_col, n_z = plan.n_col, plan.n_z
    blk, width = pieces[0][0].shape
    depth = blk * plan.n_row
    kb = depth // n_col
    rows = b2[0].shape[0] - 8 if base is None else base[0].shape[0]
    tile = 1024
    flat = [pieces[g][s] for s in slots for g in range(n_z)] + [others[g][plan.col_twin[s]] for s in slots for g in range(n_z)]
    half = n_z * len(slots)
    given = list(b2) if base is None else list(base[1:])
    more = [] if base is None else [base[0]]
    n_given = len(given)

    def body(*refs):
        b, c = refs[:n_given], refs[n_given : n_given + 2 * half]
        rest = refs[n_given + 2 * half + len(more) :]
        if base is None:
            out, both, cbuf, obuf, in_sem, out_sem = rest
        else:
            (both,), (out, cbuf, obuf, in_sem, out_sem) = b, rest
        z, core, col = plan.place()

        def fetch(s, slot):
            copies = []
            for side in range(2):
                who = core if side == 0 else 1 - core
                for g in range(n_z):
                    at = pl.multiple_of((plan.z_of(z, who, g) * 2 + who) * blk, blk)
                    copies.append(
                        pltpu.make_async_copy(
                            c[side * half + s * n_z + g],
                            cbuf.at[slot, pl.ds(at, blk), :],
                            in_sem.at[slot, len(copies)],
                        )
                    )
            return copies

        def store(s, slot):
            at = pl.multiple_of(plan.col_of(col, core, slots[s]) * width, width)
            return pltpu.make_async_copy(obuf.at[slot], out.at[:, pl.ds(at, width)], out_sem.at[slot])

        for cp in fetch(0, 0):
            cp.start()
        for s in range(n_col if base is None else 0):
            hi, lo = split3(b[s][:rows, :])
            at = pl.multiple_of(plan.col_of(col, core, s) * kb, kb)
            both[:rows, pl.ds(at, kb)] = hi
            both[rows:, pl.ds(at, kb)] = lo
        for s in range(len(slots)):
            slot = s % 2
            if s + 1 < len(slots):
                for cp in fetch(s + 1, 1 - slot):
                    cp.start()
            for cp in fetch(s, slot):
                cp.wait()
            if s >= 2:
                store(s - 2, slot).wait()

            @pl.loop(0, width // tile)
            def _(t, slot=slot):
                cols = pl.ds(pl.multiple_of(t * tile, tile), tile)
                hi, lo = split3(cbuf[slot, :, cols])
                high = jnp.dot(both[...], hi, preferred_element_type=F32)
                low = jnp.dot(both[:rows, :], lo, preferred_element_type=F32)
                obuf[slot, :, cols] = high[:rows] + (high[rows:] + low)

            store(s, slot).start()
        for s in range(max(0, len(slots) - 2), len(slots)):
            store(s, s % 2).wait()

    anywhere, near = pl.BlockSpec(memory_space=pl.ANY), pl.BlockSpec(memory_space=pltpu.VMEM)
    split, n_split = jax.ShapeDtypeStruct((2 * rows, depth), jnp.bfloat16), 1 if base is None else 0
    return pl.pallas_call(
        body,
        out_shape=[jax.ShapeDtypeStruct((rows, width * n_col), F32)] + [split] * n_split,
        in_specs=[near] * n_given + [anywhere] * len(flat + more),
        out_specs=[anywhere] + [near] * n_split,
        scratch_shapes=[
            pltpu.VMEM((2, depth, width), F32),
            pltpu.VMEM((2, rows, width), F32),
            pltpu.SemaphoreType.DMA((2, 2 * plan.n_z)),
            pltpu.SemaphoreType.DMA((2,)),
        ],
        compiler_params=pltpu.CompilerParams(vmem_limit_bytes=24 * 2**20),
        cost_estimate=pl.CostEstimate(flops=6 * rows * depth * width * len(slots), bytes_accessed=4 * (depth + rows) * width * len(slots), transcendentals=0),
        input_output_aliases={n_given + 2 * half: 0} if more else {},
    )(*given, *flat, *more)


def spread(plan, x):
    found = [x]
    for step in range(plan.col_bits):
        found = found + [plan.over_col(y, 2**step) for y in found]
    return found


def solution(mesh):
    plan = Plan(mesh)

    def per_device(basis, coef, panels, factors):
        nb, kb = panels.shape[2], basis.shape[1]
        part = panels.shape[1]
        n_col, z_bits = plan.n_col, plan.z_bits
        _, core, _ = plan.place()

        vecs = spread(plan, panels)
        sums = jnp.broadcast_to(jnp.sum(coef, axis=1)[None, :], (8, coef.shape[0]))
        for step in range(plan.col_bits):
            sums = sums + plan.over_col(sums, 2**step)

        parts = [coef]
        for step in range(z_bits):
            parts += [plan.over_z(x, 2**step) for x in parts]
        pieces = [None if plan.relayed(g) else spread(plan, x) for g, x in enumerate(parts)]
        for g, x in enumerate(parts):
            if plan.relayed(g):
                pieces[g] = [x] + [plan.over_z(pieces[0][t], g) for t in range(1, n_col)]
                pieces[g][n_col // 2] = plan.over_col(x, n_col // 2)
        others = [[plan.over_core(x) for x in found] for found in pieces]

        keep, send = project(plan, basis, vecs, sums)
        mine = keep + plan.over_core(send)
        for step in range(z_bits):
            mine = mine + plan.over_z(mine, 2**step)
        theirs = plan.over_core(mine)
        sends = update(plan, basis, vecs, factors, mine, theirs)

        tall = [sends[0]] + [plan.over_col(sends[s], s) for s in range(1, n_col)]
        shares = [x[part : part + 2 * nb // kb].reshape(2, nb) for x in tall]
        by_mask = [pick(core, [shares[m.index(i)] for m in plan.col_masks]) for i in range(n_col)]
        while len(by_mask) > 1:
            by_mask = [by_mask[i] + by_mask[i + 1] for i in range(0, len(by_mask), 2)]
        wsum = by_mask[0] / jnp.sqrt(F32(coef.shape[1] * n_col))
        first = list(range(n_col - 1))
        held = product(plan, tall, pieces, others, first)
        (vectors,) = product(plan, (), pieces, others, [n_col - 1], held)
        return vectors, wsum

    placed = (P("row", "col"), P("row", "col"), P(None, ("row", "col"), None), P())
    return jax.shard_map(
        per_device,
        mesh=mesh,
        in_specs=placed,
        out_specs=(P(("row", "col"), None), P()),
        check_vma=False,
    )
```

```python
import jax
import jax.numpy as jnp
from jax import lax
from jax.experimental import pallas as pl
from jax.experimental.pallas import tpu as pltpu
from jax.sharding import PartitionSpec as P


BOTH = ("row", "col")


F32 = jnp.float32
ROWS_ROWS = (((0,), (0,)), ((), ()))
COLS_COLS = (((1,), (1,)), ((), ()))
PLAIN = (((1,), (0,)), ((), ()))


def masks(bits, core):
    order = list(range(bits)) if core == 0 else list(range(bits))[::-1]
    out = [0]
    for b in order:
        out = out + [m ^ (1 << b) for m in out]
    return out


def split3(x):
    hi = x.astype(jnp.bfloat16)
    return hi, (x - hi.astype(F32)).astype(jnp.bfloat16)


def mul(left, right, dims=PLAIN):
    def one(a, b):
        return lax.dot_general(a, b, dims, preferred_element_type=F32)

    return one(left[0], right[0]) + (one(left[0], right[1]) + one(left[1], right[0]))


def pick(core, pair):
    return jnp.where(core == 0, pair[0], pair[1])


class Plan:
    def __init__(self, mesh):
        self.n_row, self.n_col = mesh.shape["row"], mesh.shape["col"]
        self.n_z = self.n_row // 2
        self.col_bits, self.z_bits = self.n_col.bit_length() - 1, self.n_z.bit_length() - 1
        self.col_masks = [masks(self.col_bits, core) for core in range(2)]
        self.z_masks = [masks(self.z_bits, core) for core in range(2)]
        self.col_twin = [self.col_masks[1].index(m) for m in self.col_masks[0]]

    def relayed(self, slot):
        return self.n_z > 2 and self.n_col > 2 and slot == self.n_z // 2

    def place(self):
        row, col = lax.axis_index("row"), lax.axis_index("col")
        return row // 2, lax.rem(row, 2), col

    def col_of(self, col, core, slot):
        return col ^ pick(core, [m[slot] for m in self.col_masks])

    def z_of(self, z, core, slot):
        return z ^ pick(core, [m[slot] for m in self.z_masks])

    def permute(self, x, to):
        pairs = [(r * self.n_col + c, to(r, c)) for r in range(self.n_row) for c in range(self.n_col)]
        return lax.ppermute(x, BOTH, pairs)

    def over_col(self, x, slot):
        return self.permute(x, lambda r, c: r * self.n_col + (c ^ self.col_masks[r % 2][slot]))

    def over_z(self, x, slot):
        return self.permute(x, lambda r, c: (r ^ (2 * self.z_masks[r % 2][slot])) * self.n_col + c)

    def over_core(self, x):
        return self.permute(x, lambda r, c: (r ^ 1) * self.n_col + c)


def project(plan, basis, vecs, sums):
    n_col, kb = plan.n_col, basis.shape[1]
    part, nb = vecs[0].shape[1:]
    half = kb // 2
    blk = sums.shape[1]
    cuts = nb // kb
    height = (2 + cuts) * nb + 8

    def body(basis_ref, sums_ref, *refs):
        v, (keep, send, total) = refs[:n_col], refs[n_col:]
        z, core, col = plan.place()
        proj, cross = [0.0, 0.0], 0.0
        for s in range(n_col):
            at = pl.multiple_of(plan.col_of(col, core, s) * part, part)
            b = split3(basis_ref[pl.ds(at, part), :])
            v0, v1 = split3(v[s][0]), split3(v[s][1])
            proj[0] += mul(v0, b, ROWS_ROWS)
            proj[1] += mul(v1, b, ROWS_ROWS)
            cross += mul(v1, v0, ROWS_ROWS)
        total[:nb, :] = proj[0]
        total[nb : 2 * nb, :] = proj[1]
        for i in range(cuts):
            total[(2 + i) * nb : (3 + i) * nb, :] = cross[:, i * kb : (i + 1) * kb]
        per = kb // blk if kb >= blk else 1
        line = lax.broadcasted_iota(jnp.int32, (8, kb), 0) * per + lax.broadcasted_iota(jnp.int32, (8, kb), 1) // blk
        wide = jnp.concatenate([sums_ref[:1, :]] * per, axis=1)
        total[height - 8 :, :] = jnp.where(line == z * 2 + core, jnp.broadcast_to(wide, (8, kb)), 0.0)
        left, right = total[:, :half], total[:, half:]
        keep[...] = jnp.where(core == 0, left, right)
        send[...] = jnp.where(core == 0, right, left)

    out = jax.ShapeDtypeStruct((height, half), F32)
    return pl.pallas_call(
        body,
        out_shape=(out, out),
        scratch_shapes=[pltpu.VMEM((height, kb), F32)],
        compiler_params=pltpu.CompilerParams(vmem_limit_bytes=16 * 2**20),
        cost_estimate=pl.CostEstimate(flops=36 * part * n_col * nb * kb, bytes_accessed=4 * (3 * part * n_col * kb + height * kb), transcendentals=0),
        name="project",
    )(basis, sums, *vecs)


def update(plan, basis, vecs, factors, mine, theirs):
    n_col, kb = plan.n_col, basis.shape[1]
    part, nb = vecs[0].shape[1:]
    height, _ = mine.shape
    cuts = nb // kb
    tail = 8

    def body(basis_ref, factors_ref, mine_ref, theirs_ref, *refs):
        v, outs = refs[:n_col], refs[n_col:]
        _, core, col = plan.place()
        left = jnp.where(core == 0, mine_ref[...], theirs_ref[...])
        right = jnp.where(core == 0, theirs_ref[...], mine_ref[...])
        total = jnp.concatenate([left, right], axis=1)
        keep = lax.broadcasted_iota(jnp.int32, (nb, nb), 0) <= lax.broadcasted_iota(jnp.int32, (nb, nb), 1)
        upper = [split3(jnp.where(keep, factors_ref[i], 0.0)) for i in range(2)]
        one, two = total[:nb], total[nb : 2 * nb]
        cross = jnp.concatenate([total[(2 + i) * nb : (3 + i) * nb] for i in range(cuts)], axis=1)
        first = mul(upper[0], split3(one))
        split_first = split3(first)
        two = two - mul(split3(cross), split_first)
        split_second = split3(mul(upper[1], split3(two)))
        line = lax.broadcasted_iota(jnp.int32, (8, kb), 0)
        weight = jnp.sum(jnp.where(line == col, total[height - 8 :], 0.0), axis=0, keepdims=True)
        weight = split3(jnp.broadcast_to(weight, (8, kb)))
        shares = [mul(weight, split3(g), COLS_COLS)[:1] for g in (one, two)]
        shares = [x[:, i * kb : (i + 1) * kb] for x in shares for i in range(cuts)]
        shares = jnp.concatenate(shares + [jnp.zeros((tail - 2 * cuts, kb), F32)], axis=0)
        for s in range(n_col):
            at = pl.multiple_of(plan.col_of(col, core, s) * part, part)
            b = basis_ref[pl.ds(at, part), :]
            b = b - mul(split3(v[s][0]), split_first) - mul(split3(v[s][1]), split_second)
            outs[s][:part, :] = b
            outs[s][part:, :] = shares

    out = jax.ShapeDtypeStruct((part + tail, kb), F32)
    return pl.pallas_call(
        body,
        out_shape=(out,) * n_col,
        compiler_params=pltpu.CompilerParams(vmem_limit_bytes=16 * 2**20),
        cost_estimate=pl.CostEstimate(flops=12 * part * n_col * nb * kb, bytes_accessed=4 * (4 * part * n_col * kb + height * kb), transcendentals=0),
        name="update",
    )(basis, factors, mine, theirs, *vecs)


def product(plan, b2, pieces, others, slots, lines, base=None):
    n_col, n_z = plan.n_col, plan.n_z
    blk, width = pieces[0][0].shape
    depth = blk * plan.n_row
    kb = depth // n_col
    rows = b2[0].shape[0] - 8 if base is None else base[0].shape[0]
    tile = 1024
    flat = [pieces[g][s] for s in slots for g in range(n_z)] + [others[g][plan.col_twin[s]] for s in slots for g in range(n_z)]
    half = n_z * len(slots)
    given = list(b2) if base is None else list(base[1:])
    more = [] if base is None else [base[0]]
    n_given = len(given)

    def body(*refs):
        b, c = refs[:n_given], refs[n_given : n_given + 2 * half]
        rest = refs[n_given + 2 * half + len(more) :]
        if base is None:
            out, both, wsum, cbuf, obuf, in_sem, out_sem = rest
        else:
            (both,), (out, cbuf, obuf, in_sem, out_sem) = b, rest
        z, core, col = plan.place()

        def fetch(s, slot):
            copies = []
            for side in range(2):
                who = core if side == 0 else 1 - core
                for g in range(n_z):
                    at = pl.multiple_of((plan.z_of(z, who, g) * 2 + who) * blk, blk)
                    copies.append(
                        pltpu.make_async_copy(
                            c[side * half + s * n_z + g],
                            cbuf.at[slot, pl.ds(at, blk), :],
                            in_sem.at[slot, len(copies)],
                        )
                    )
            return copies

        def store(s, slot):
            at = pl.multiple_of(plan.col_of(col, core, slots[s]) * width, width)
            return pltpu.make_async_copy(obuf.at[slot], out.at[:, pl.ds(at, width)], out_sem.at[slot])

        for cp in fetch(0, 0):
            cp.start()
        for s in range(n_col if base is None else 0):
            hi, lo = split3(b[s][:rows, :])
            at = pl.multiple_of(plan.col_of(col, core, s) * kb, kb)
            both[:rows, pl.ds(at, kb)] = hi
            both[rows:, pl.ds(at, kb)] = lo
        if base is None:
            shares = [ref[rows : rows + lines, :] for ref in b]
            shares = [pick(core, [shares[m.index(i)] for m in plan.col_masks]) for i in range(n_col)]
            while len(shares) > 1:
                shares = [shares[i] + shares[i + 1] for i in range(0, len(shares), 2)]
            wsum[...] = shares[0] / jnp.sqrt(F32(width * n_col))
        for s in range(len(slots)):
            slot = s % 2
            if s + 1 < len(slots):
                for cp in fetch(s + 1, 1 - slot):
                    cp.start()
            for cp in fetch(s, slot):
                cp.wait()
            if s >= 2:
                store(s - 2, slot).wait()

            @pl.loop(0, width // tile)
            def _(t, slot=slot):
                cols = pl.ds(pl.multiple_of(t * tile, tile), tile)
                hi, lo = split3(cbuf[slot, :, cols])
                high = jnp.dot(both[...], hi, preferred_element_type=F32)
                low = jnp.dot(both[:rows, :], lo, preferred_element_type=F32)
                obuf[slot, :, cols] = high[:rows] + (high[rows:] + low)

            store(s, slot).start()
        for s in range(max(0, len(slots) - 2), len(slots)):
            store(s, s % 2).wait()

    anywhere, near = pl.BlockSpec(memory_space=pl.ANY), pl.BlockSpec(memory_space=pltpu.VMEM)
    extra = [jax.ShapeDtypeStruct((2 * rows, depth), jnp.bfloat16), jax.ShapeDtypeStruct((lines, kb), F32)]
    extra = extra if base is None else []
    return pl.pallas_call(
        body,
        out_shape=[jax.ShapeDtypeStruct((rows, width * n_col), F32)] + extra,
        in_specs=[near] * n_given + [anywhere] * len(flat + more),
        out_specs=[anywhere] + [near] * len(extra),
        scratch_shapes=[
            pltpu.VMEM((2, depth, width), F32),
            pltpu.VMEM((2, rows, width), F32),
            pltpu.SemaphoreType.DMA((2, 2 * plan.n_z)),
            pltpu.SemaphoreType.DMA((2,)),
        ],
        compiler_params=pltpu.CompilerParams(vmem_limit_bytes=24 * 2**20),
        cost_estimate=pl.CostEstimate(flops=6 * rows * depth * width * len(slots), bytes_accessed=4 * (depth + rows) * width * len(slots), transcendentals=0),
        input_output_aliases={n_given + 2 * half: 0} if more else {},
    )(*given, *flat, *more)


def spread(plan, x):
    found = [x]
    for step in range(plan.col_bits):
        found = found + [plan.over_col(y, 2**step) for y in found]
    return found


def solution(mesh):
    plan = Plan(mesh)

    def per_device(basis, coef, panels, factors):
        nb, kb = panels.shape[2], basis.shape[1]
        n_col, z_bits = plan.n_col, plan.z_bits
        z, core, col = plan.place()

        vecs = spread(plan, panels)
        sums = jnp.broadcast_to(jnp.sum(coef, axis=1)[None, :], (8, coef.shape[0]))
        for step in range(plan.col_bits):
            sums = sums + plan.over_col(sums, 2**step)

        parts = [coef]
        for step in range(z_bits):
            parts += [plan.over_z(x, 2**step) for x in parts]
        pieces = [None if plan.relayed(g) else spread(plan, x) for g, x in enumerate(parts)]
        for g, x in enumerate(parts):
            if plan.relayed(g):
                pieces[g] = [x] + [plan.over_z(pieces[0][t], g) for t in range(1, n_col)]
                pieces[g][n_col // 2] = plan.over_col(x, n_col // 2)
        others = [[plan.over_core(x) for x in found] for found in pieces]

        keep, send = project(plan, basis, vecs, sums)
        mine = keep + plan.over_core(send)
        for step in range(z_bits):
            mine = mine + plan.over_z(mine, 2**step)
        theirs = plan.over_core(mine)
        sends = update(plan, basis, vecs, factors, mine, theirs)

        tall = [sends[0]] + [plan.over_col(sends[s], s) for s in range(1, n_col)]
        lines = 2 * nb // kb
        first = list(range(n_col - 1))
        *held, wsum = product(plan, tall, pieces, others, first, lines)
        (vectors,) = product(plan, (), pieces, others, [n_col - 1], lines, held)
        return vectors, wsum.reshape(2, nb)

    placed = (P("row", "col"), P("row", "col"), P(None, ("row", "col"), None), P())
    return jax.shard_map(
        per_device,
        mesh=mesh,
        in_specs=placed,
        out_specs=(P(("row", "col"), None), P()),
        check_vma=False,
    )
```
